32 devices in a mesh: dp: 8 (over z, y), mp: 4 (over x, core).
Axes of the slice: x: 2, y: 2, z: 4, core: 2. Of those that a mesh axis runs over, the one named last changes fastest.
Arguments:
- patch_query: bfloat16 [2048, 4096], P('dp'), may hold values from -6 to 6
- key_cache: bfloat16 [2048, 16, 4096], P('dp', None, 'mp'), may hold values from -48 to 48
- value_cache: bfloat16 [2048, 16, 4096], P('dp', None, 'mp'), may hold values from -6 to 6
- cache_len: int32 [2048], P('dp'), may hold values from 1 to 16
- patch_end: int32 [2048], P('dp'), may hold values from 0 to 1, as said below
- ended_index: int32 [1024], P('dp'), may hold values from 0 to 256, as said below
- pool_out: bfloat16 [4096, 4096], P('mp'), may hold values from -0.09375 to 0.09375
- norm_gain: float32 [2, 4096], replicated, may hold values from 0.1 to 1.9
- w_in: bfloat16 [2, 4096, 2, 14336], P(None, 'dp', None, 'mp'), may hold values from -0.09375 to 0.09375
- w_out: bfloat16 [2, 14336, 4096], P(None, 'mp', 'dp'), may hold values from -0.046875 to 0.046875
Outputs:
- global_out: bfloat16 [2048, 4096], P('dp')
The draws below stay inside these ranges and needn't reach their ends.
Inputs may be any that keep to these rules, and one draw needn't show every extreme that they name: `patch_end`: each index of dp has at most 128 ended patches among its 256 sequences, and some index has exactly 128. `ended_index`: each aligned block of 128 entries lists, in increasing order, the local indices of the ended sequences of that index of dp, then 256 in the remaining entries.
All inputs are finite; a program needn't handle non-finite values.
Results may differ from the reference program's by a relative error of at most 0.024.
Values may be sent and summed in bfloat16 or wider, within the bound.
A program may use at most 128 MiB of HBM per device.

```python
import jax
import jax.numpy as jnp
from jax import lax

D = 4096
FF = 14336
HEAD_DIM = 128
LAYERS = 2
PATCH = 16
SEQ_DEV = 256
CAP = 128
B = 2048
R = 1024
N_DP = 8
N_MP = 4


def query_and_keys(key):
    query_draw = jnp.clip(jax.random.normal(jax.random.fold_in(key, 11), (B, D), jnp.float32), -6.0, 6.0)
    keys_draw = jnp.clip(jax.random.normal(jax.random.fold_in(key, 12), (B, PATCH, D), jnp.float32), -6.0, 6.0)
    return (query_draw, keys_draw)


def draw_patch_query(key, part):
    return query_and_keys(key)[0].astype(jnp.bfloat16)


def draw_key_cache(key, part):
    return query_and_keys(key)[1].astype(jnp.bfloat16)


def ended_tables(key):
    shards = B // SEQ_DEV
    shard_keys = jax.random.split(jax.random.fold_in(key, 21), shards)
    counts = jax.random.randint(jax.random.fold_in(key, 22), (shards,), CAP // 4, CAP + 1)
    fullest = jax.random.randint(jax.random.fold_in(key, 23), (), 0, shards)
    counts = counts.at[fullest].set(CAP)

    def single_shard(shard_key, ended_count):
        permuted = jax.random.permutation(shard_key, SEQ_DEV)
        ranking = jnp.argsort(permuted, stable=True)
        flagged = (ranking < ended_count).astype(jnp.int32)
        position = jnp.cumsum(flagged) - 1
        target = jnp.where(flagged == 1, position, CAP)
        slot_index = jnp.full((CAP,), SEQ_DEV, jnp.int32).at[target].set(jnp.arange(SEQ_DEV, dtype=jnp.int32), mode='drop')
        return (flagged, slot_index)
    flagged, slot_index = jax.vmap(single_shard)(shard_keys, counts)
    return (flagged.reshape(-1).astype(jnp.int32), slot_index.reshape(-1).astype(jnp.int32))


def draw_patch_end(key, part):
    return ended_tables(key)[0]


def draw_ended_index(key, part):
    return ended_tables(key)[1]


def plant(drawn, rng, smallest, largest):
    index_at = [jax.random.randint(jax.random.fold_in(rng, axis), (), 0, length) for axis, length in enumerate(drawn.shape)]
    longest = drawn.shape.index(max(drawn.shape))
    beside = index_at[:longest] + [(index_at[longest] + 1) % drawn.shape[longest]] + index_at[longest + 1:]
    return drawn.at[tuple(index_at)].set(smallest).at[tuple(beside)].set(largest)


def levels(stream_key, dims, pieces, low, largest):
    factor_of, own = 1.0, jax.random.fold_in(stream_key, 6)
    for dim, parts in pieces:
        draws = jnp.exp(jax.random.uniform(jax.random.fold_in(own, dim), (parts,), jnp.float32, low / len(pieces), largest / len(pieces)))
        factor_of = factor_of * jnp.repeat(draws, dims[dim] // parts).reshape([-1 if axis == dim else 1 for axis in range(len(dims))])
    return factor_of


def gaussian(rng, dims, scale, most, pieces=(), held_as=jnp.bfloat16):
    values = scale * jax.random.normal(rng, dims, jnp.float32)
    if pieces:
        values = values * levels(rng, dims, pieces, -0.22, 0.18)
    return jnp.clip(values, -most, most).astype(held_as)


def setup_inputs(seed: int = 0) -> dict:
    streams_of = jax.random.split(jax.random.key(seed), 11)
    return {
        "patch_query": draw_patch_query(jax.random.fold_in(streams_of[10], 71), 0),
        "key_cache": draw_key_cache(jax.random.fold_in(streams_of[10], 71), 0),
        "value_cache": gaussian(streams_of[2], (B, PATCH, D), 1.0, 6.0, ((0, 8), (2, 4))),
        "cache_len": plant(jax.random.randint(streams_of[3], (B,), 1, PATCH + 1), jax.random.fold_in(streams_of[3], 1), 1, PATCH).astype(jnp.int32),
        "patch_end": draw_patch_end(jax.random.fold_in(streams_of[10], 71), 0),
        "ended_index": draw_ended_index(jax.random.fold_in(streams_of[10], 71), 0),
        "pool_out": gaussian(streams_of[6], (D, D), D ** -0.5, 0.09375, ((0, 4),)),
        "norm_gain": jnp.clip(1.0 + 0.18 * jax.random.normal(streams_of[7], (LAYERS, D), jnp.float32), 0.1, 1.9),
        "w_in": gaussian(streams_of[8], (LAYERS, D, 2, FF), D ** -0.5, 0.09375, ((1, 8), (3, 4))),
        "w_out": gaussian(streams_of[9], (LAYERS, FF, D), FF ** -0.5, 0.046875, ((1, 4), (2, 8))),
    }


norm_floor = 1e-05

def rounded(value):
    return lax.optimization_barrier(value.astype(jnp.bfloat16)).astype(jnp.float32)

def attend_all(query, keys, values, lengths):
    total_rows, patch_len, full_width = keys.shape
    head_count = full_width // HEAD_DIM
    query_heads = query.astype(jnp.float32).reshape(total_rows, head_count, HEAD_DIM)
    key_heads = keys.astype(jnp.float32).reshape(total_rows, patch_len, head_count, HEAD_DIM)
    value_heads = values.astype(jnp.float32).reshape(total_rows, patch_len, head_count, HEAD_DIM)
    scores = jnp.einsum('shd,sphd->shp', query_heads, key_heads, precision=lax.Precision.HIGHEST) * HEAD_DIM ** (-0.5)
    live_mask = jnp.arange(patch_len, dtype=jnp.int32)[None, None, :] < lengths[:, None, None]
    scores = jnp.where(live_mask, scores, jnp.float32(-1e+30))
    top_score = lax.optimization_barrier(jnp.max(scores, axis=2, keepdims=True))
    expo = jnp.where(live_mask, jnp.exp(scores - top_score), jnp.float32(0.0))
    weights = (expo / lax.optimization_barrier(jnp.sum(expo, axis=2, keepdims=True))).astype(jnp.bfloat16)
    mixed = jnp.einsum('shp,sphd->shd', weights.astype(jnp.float32), value_heads, precision=lax.Precision.HIGHEST)
    return mixed.astype(jnp.bfloat16).reshape(total_rows, full_width)

def blocked_product(left, right, blocks):
    rows = left.shape[0]
    inner = left.shape[1] // blocks
    left_blocks = left.reshape(rows, blocks, inner)
    right_blocks = right.reshape(blocks, inner, right.shape[1])

    def add_block(index, carry):
        left_part = lax.dynamic_index_in_dim(left_blocks, index, 1, keepdims=False).astype(jnp.float32)
        right_part = lax.dynamic_index_in_dim(right_blocks, index, 0, keepdims=False).astype(jnp.float32)
        term = jnp.dot(left_part, right_part, precision=lax.Precision.HIGHEST, preferred_element_type=jnp.float32)
        return carry + rounded(term)
    start_value = jnp.zeros((rows, right.shape[1]), jnp.float32)
    return lax.fori_loop(0, blocks, add_block, start_value)

def reference(patch_query, key_cache, value_cache, cache_len, patch_end, ended_index, pool_out, norm_gain, w_in, w_out):
    attended = attend_all(patch_query, key_cache, value_cache, cache_len)
    pooled = patch_query.astype(jnp.float32) + blocked_product(attended, pool_out, N_MP)
    owner = jnp.arange(R, dtype=jnp.int32) // CAP
    valid = ended_index < SEQ_DEV
    rows = (owner * SEQ_DEV + jnp.minimum(ended_index, SEQ_DEV - 1)).astype(jnp.int32)
    state = jnp.where(valid[:, None], pooled[rows], jnp.float32(0.0))
    for layer_idx in range(LAYERS):
        mean_square = lax.optimization_barrier(jnp.mean(state * state, axis=1, keepdims=True))
        normed = (state * lax.rsqrt(mean_square + norm_floor) * norm_gain[layer_idx][None, :]).astype(jnp.bfloat16)
        gate_up = blocked_product(normed, w_in[layer_idx].reshape(D, 2 * FF), N_DP)
        hidden = (jax.nn.silu(gate_up[:, :FF]) * gate_up[:, FF:]).astype(jnp.bfloat16)
        ffn = blocked_product(hidden, w_out[layer_idx], N_MP).astype(jnp.bfloat16)
        state = state + ffn.astype(jnp.float32)
    placed = jnp.zeros((B, D), jnp.float32).at[rows].add(jnp.where(valid[:, None], state, jnp.float32(0.0)))
    return (placed * patch_end.astype(jnp.float32)[:, None]).astype(jnp.bfloat16)
```

```python
import jax
import jax.numpy as jnp
from jax import lax
from jax.sharding import PartitionSpec as P

HEAD_DIM = 128


norm_floor = 1e-05


def attend_local(query_cols, keys, values, lengths):
    seq_rows, patch_len, heads_width = keys.shape
    head_count = heads_width // HEAD_DIM
    query_heads = query_cols.reshape(seq_rows, head_count, HEAD_DIM)
    key_heads = keys.reshape(seq_rows, patch_len, head_count, HEAD_DIM)
    value_heads = values.reshape(seq_rows, patch_len, head_count, HEAD_DIM)
    scores = jnp.einsum(
        "shd,sphd->shp", query_heads, key_heads, preferred_element_type=jnp.float32
    ) * HEAD_DIM ** (-0.5)
    live_mask = jnp.arange(patch_len, dtype=jnp.int32)[None, None, :] < lengths[:, None, None]
    scores = jnp.where(live_mask, scores, jnp.float32(-1e30))
    top_score = jnp.max(scores, axis=2, keepdims=True)
    expo = jnp.where(live_mask, jnp.exp(scores - top_score), jnp.float32(0.0))
    weights = (expo / jnp.sum(expo, axis=2, keepdims=True)).astype(jnp.bfloat16)
    mixed = jnp.einsum("shp,sphd->shd", weights, value_heads, preferred_element_type=jnp.float32)
    return mixed.astype(jnp.bfloat16).reshape(seq_rows, heads_width)


def shift(value, size, step):
    return lax.ppermute(value, "dp", [(i, (i + step) % size) for i in range(size)])


def swap(value, axis, size, bit):
    return lax.ppermute(value, axis, [(i, i ^ bit) for i in range(size)])


def sum_over_mp(value, size):
    if size & (size - 1) or size < 2:
        return lax.psum(value, "mp").astype(jnp.float32)
    low = lax.axis_index("mp") % 2
    half = value.shape[0] // 2
    kept = lax.dynamic_slice_in_dim(value, low * half, half, 0)
    given = lax.dynamic_slice_in_dim(value, (1 - low) * half, half, 0)
    total = kept.astype(jnp.float32) + swap(given, "mp", size, 1).astype(jnp.float32)
    bit = 2
    while bit < size:
        sent = total.astype(jnp.bfloat16)
        total = sent.astype(jnp.float32) + swap(sent, "mp", size, bit).astype(jnp.float32)
        bit *= 2
    mine = total.astype(jnp.bfloat16)
    other = swap(mine, "mp", size, 1)
    lower = jnp.where(low == 0, mine, other)
    upper = jnp.where(low == 0, other, mine)
    return jnp.concatenate([lower, upper], axis=0).astype(jnp.float32)


def mix(n_dp, n_mp, *args):
    (patch_query, key_cache, value_cache, cache_len, patch_end, ended_index, pool_out, norm_gain, w_in, w_out) = args
    layers, block_cols, _, hidden_local = w_in.shape
    ring = n_dp // 2
    half = hidden_local // 2
    place = lax.axis_index("dp")
    ring_at, side = place // 2, place % 2

    in_own, in_other, out_own, out_other = [], [], [], []
    for layer_idx in range(layers):
        def in_half(which):
            return lax.dynamic_slice_in_dim(w_in[layer_idx], which * half, half, 2).reshape(block_cols, 2 * half)

        def out_half(which):
            return lax.dynamic_slice_in_dim(w_out[layer_idx], which * half, half, 0)

        in_own.append(in_half(side))
        in_other.append(swap(in_half(1 - side), "dp", n_dp, 1))
        out_own.append(out_half(side))
        out_other.append(swap(out_half(1 - side), "dp", n_dp, 1))

    seq_rows = patch_query.shape[0]
    heads_width = key_cache.shape[2]
    col_start = lax.axis_index("mp") * heads_width
    query_cols = lax.dynamic_slice_in_dim(patch_query, col_start, heads_width, 1)
    attended = attend_local(query_cols, key_cache, value_cache, cache_len)
    picker = (ended_index[:, None] == jnp.arange(seq_rows, dtype=jnp.int32)[None, :]).astype(
        jnp.float32
    )
    picker_half = picker.astype(jnp.bfloat16)
    chosen = jnp.dot(picker_half, attended, preferred_element_type=jnp.float32).astype(jnp.bfloat16)
    partial_value = jnp.dot(chosen, pool_out, preferred_element_type=jnp.float32)
    pooled_sum = sum_over_mp(partial_value.astype(jnp.bfloat16), n_mp)
    query_rows = jnp.dot(picker_half, patch_query, preferred_element_type=jnp.float32)
    residual = query_rows + pooled_sum
    rows = residual.shape[0]
    width = 2 * block_cols
    for layer_idx in range(layers):
        mean_square = jnp.mean(residual * residual, axis=1, keepdims=True)
        normed = (
            residual * lax.rsqrt(mean_square + norm_floor) * norm_gain[layer_idx][None, :]
        ).astype(jnp.bfloat16)
        spread = []
        for step in range(ring):
            target = (ring_at + step) % ring
            piece = lax.dynamic_slice_in_dim(normed, target * width, width, 1)
            spread.append(piece if step == 0 else shift(piece, n_dp, 2 * step))
        carried = None
        for step in range(ring):
            held = spread[(step + 1) % ring]
            both = jnp.concatenate([held, swap(held, "dp", n_dp, 1)], axis=0)
            feats_own = lax.dynamic_slice_in_dim(both, side * block_cols, block_cols, 1)
            feats_other = lax.dynamic_slice_in_dim(both, (1 - side) * block_cols, block_cols, 1)
            term = jnp.dot(feats_own, in_own[layer_idx], preferred_element_type=jnp.float32)
            term = term + jnp.dot(feats_other, in_other[layer_idx], preferred_element_type=jnp.float32)
            if carried is not None:
                term = term + carried.astype(jnp.float32)
            if step < ring - 1:
                carried = shift(term.astype(jnp.bfloat16), n_dp, 2)
        hidden = (jax.nn.silu(term[:, :half]) * term[:, half:]).astype(jnp.bfloat16)
        pieces = []
        for step in range(ring):
            following = shift(hidden, n_dp, 2) if step < ring - 1 else None
            cols_own = jnp.dot(hidden, out_own[layer_idx], preferred_element_type=jnp.float32)
            cols_other = jnp.dot(hidden, out_other[layer_idx], preferred_element_type=jnp.float32)
            given = jnp.concatenate([cols_other[rows:], cols_own[rows:]], axis=1).astype(jnp.bfloat16)
            kept = jnp.concatenate([cols_own[:rows], cols_other[:rows]], axis=1)
            piece = (kept + swap(given, "dp", n_dp, 1).astype(jnp.float32)).astype(jnp.bfloat16)
            pieces.append(piece if step == 0 else shift(piece, n_dp, (-2 * step) % n_dp))
            hidden = following
        twice = jnp.concatenate(pieces + pieces, axis=1)
        ordered = lax.dynamic_slice_in_dim(twice, (ring - ring_at) * width, ring * width, 1)
        summed = sum_over_mp(ordered, n_mp).reshape(rows, ring, 2, block_cols)
        summed = jnp.where(side == 0, summed, summed[:, :, ::-1, :]).reshape(rows, ring * width)
        residual = residual + summed.astype(jnp.bfloat16).astype(jnp.float32)
    placed = jnp.dot(
        picker.T, residual, precision=lax.Precision.HIGHEST, preferred_element_type=jnp.float32
    )
    return (placed * patch_end.astype(jnp.float32)[:, None]).astype(jnp.bfloat16)


def solution(mesh):
    in_specs = (
        P("dp", None),
        P("dp", None, "mp"),
        P("dp", None, "mp"),
        P("dp"),
        P("dp"),
        P("dp"),
        P("mp", None),
        P(),
        P(None, "dp", None, "mp"),
        P(None, "mp", "dp"),
    )
    out_specs = P("dp", None)
    def per_device(*args):
        return mix(mesh.shape["dp"], mesh.shape["mp"], *args)

    return jax.shard_map(
        per_device, mesh=mesh, in_specs=in_specs, out_specs=out_specs, check_vma=False
    )
```
